16 devices in a mesh: dp: 2 (over y, z), pp: 8 (over x, core).
Axes of the slice: x: 4, y: 2, z: 1, core: 2. Of those that a mesh axis runs over, the one named last changes fastest.
The devices are a block of a 4x4x8 slice.
Arguments:
- hidden: bfloat16 [32, 512, 2048], P(('dp', 'pp')), parts along dimension 0
- labels: int32 [32, 512], P(('dp', 'pp')), parts along dimension 0
- gamma: float32 [2048], replicated
- table: bfloat16 [49152, 2048], P('pp')
Outputs:
- output 1: float32 [32, 512], P(('dp', 'pp')), parts along dimension 0
- output 2: bfloat16 [32, 512, 2048], P(('dp', 'pp')), parts along dimension 0
- output 3: float32 [2], P('dp'), parts along dimension 0
- output 4: float32 [98304, 2048], P(('dp', 'pp')), parts along dimension 0
- output 5: float32 [4096], P('dp'), parts along dimension 0
There are 2 independent parts. The reference program is written for one: setup_inputs(seed, part) draws one part's arguments, and reference() takes and returns one part's arrays. A program takes and returns all parts, laid end to end along the dimension named above; an argument that names none is the same for every part.
All inputs are finite; a program needn't handle non-finite values.
Results may differ from the reference program's by a relative error of at most 0.001.
Values are sent between devices in bfloat16 or wider.
A program may use at most 768 MiB of HBM per device.

```python
import jax
import jax.numpy as jnp
from jax import lax

MICROBATCHES = 16
SEQ_LEN = 512
D_MODEL = 2048
VOCAB_SIZE = 49152
SOFT_CAP = 30
EPS = 1e-6
LOGIT_SCALE = 10.0


def setup_inputs(seed: int = 0, part: int = 0) -> dict:
    base_key = jax.random.key(seed)
    shared_key, part_base = jax.random.split(base_key)
    part_key = jax.random.fold_in(part_base, part)
    key_hidden, key_labels = jax.random.split(part_key)
    key_gain, key_table = jax.random.split(shared_key)
    hidden = jax.random.normal(key_hidden, (MICROBATCHES, SEQ_LEN, D_MODEL), jnp.float32).astype(jnp.bfloat16)
    labels = jax.random.randint(key_labels, (MICROBATCHES, SEQ_LEN), 0, VOCAB_SIZE, dtype=jnp.int32)
    gamma = 0.3 * jax.random.normal(key_gain, (D_MODEL,), jnp.float32)
    table_f = jax.random.normal(key_table, (VOCAB_SIZE, D_MODEL), jnp.float32) * (LOGIT_SCALE * D_MODEL ** -0.5)
    return {'hidden': hidden, 'labels': labels, 'gamma': gamma, 'table': table_f.astype(jnp.bfloat16)}


def norm_rows(rows, gain):
    mean_sq = jnp.mean(rows * rows, axis=-1, keepdims=True)
    return rows * lax.rsqrt(mean_sq + EPS) * (1.0 + gain)


def reference(hidden, labels, gamma, table):
    total = MICROBATCHES * SEQ_LEN
    vocab_ids = lax.broadcasted_iota(jnp.int32, (1, VOCAB_SIZE), 1)

    def micro_step(carry, scan_in):
        grad_table, grad_gain = carry
        block, block_labels = scan_in
        normed32, norm_vjp = jax.vjp(norm_rows, block.astype(jnp.float32), gamma)
        normed = normed32.astype(jnp.bfloat16)
        logits = jnp.dot(normed, table.T, preferred_element_type=jnp.float32)
        tanh_z = jnp.tanh(logits / SOFT_CAP)
        capped = SOFT_CAP * tanh_z
        row_max = jnp.max(capped, axis=1, keepdims=True)
        log_norm = row_max + jnp.log(jnp.sum(jnp.exp(capped - row_max), axis=1, keepdims=True))
        label_hit = vocab_ids == block_labels[:, None]
        label_logit = jnp.sum(jnp.where(label_hit, capped, 0.0), axis=1)
        tok_loss = log_norm[:, 0] - label_logit
        soft_probs = jnp.exp(capped - log_norm)
        grad_capped = jnp.where(label_hit, soft_probs - 1.0, soft_probs) / total
        grad_logits = (grad_capped * (1.0 - tanh_z * tanh_z)).astype(jnp.bfloat16)
        grad_normed = jnp.dot(grad_logits, table, preferred_element_type=jnp.float32)
        grad_block, gain_part = norm_vjp(grad_normed)
        table_part = jnp.dot(grad_logits.T, normed, preferred_element_type=jnp.float32)
        return (grad_table + table_part, grad_gain + gain_part), (tok_loss, grad_block.astype(jnp.bfloat16))

    init_acc = (jnp.zeros((VOCAB_SIZE, D_MODEL), jnp.float32), jnp.zeros((D_MODEL,), jnp.float32))
    (grad_table, grad_gain), (tok_loss, grad_hidden) = lax.scan(micro_step, init_acc, (hidden, labels))
    mean_loss = jnp.reshape(jnp.mean(tok_loss), (1,))
    return tok_loss, grad_hidden, mean_loss, grad_table, grad_gain
```

```python
import jax
import jax.numpy as jnp
from jax import lax
from jax.sharding import PartitionSpec as P

SOFT_CAP = 30.0
EPS = 1e-6
CHUNKS = 4


def norm_rows(rows, gain):
    mean_sq = jnp.mean(rows * rows, axis=-1, keepdims=True)
    return rows * lax.rsqrt(mean_sq + EPS) * (1.0 + gain)


def solution(mesh):
    group = mesh.shape['pp']

    def local_fn(hidden, labels, gamma, table):
        mb_dev, seq_len, width = hidden.shape
        rows_dev = mb_dev * seq_len
        total = rows_dev * group
        part = rows_dev // CHUNKS
        v_shard = table.shape[0]
        rank = lax.axis_index('pp')
        rows = hidden.reshape(rows_dev, width)
        normed32, norm_vjp = jax.vjp(norm_rows, rows.astype(jnp.float32), gamma)
        normed = normed32.astype(jnp.bfloat16)
        all_labels = lax.all_gather(labels.reshape(rows_dev), 'pp', axis=0, tiled=False)
        vocab_ids = rank * v_shard + lax.broadcasted_iota(jnp.int32, (1, v_shard), 1)

        blocks = [lax.all_gather(normed[i * part:(i + 1) * part], 'pp', axis=0, tiled=True) for i in range(CHUNKS)]
        grad_table = None
        own_dn, own_loss, loss_sum = [], [], 0.0
        for i in range(CHUNKS):
            block = blocks[i]
            block_labels = all_labels[:, i * part:(i + 1) * part].reshape(group * part)
            label_hit = vocab_ids == block_labels[:, None]
            logits = lax.dot_general(block, table, (((1,), (1,)), ((), ())), preferred_element_type=jnp.float32)
            capped = SOFT_CAP * jnp.tanh(logits / SOFT_CAP)
            local_stats = jnp.stack([jnp.sum(jnp.exp(capped), axis=1),
                                     jnp.sum(jnp.where(label_hit, capped, 0.0), axis=1)])
            logits, local_stats = lax.optimization_barrier((logits, local_stats))
            stats = lax.psum(local_stats, 'pp')
            tok_loss = jnp.log(stats[0]) - stats[1]
            scale = 1.0 / (stats[0] * total)
            tanh_z = jnp.tanh(logits / SOFT_CAP)
            probs = jnp.exp(SOFT_CAP * tanh_z) * scale[:, None]
            grad_capped = jnp.where(label_hit, probs - 1.0 / total, probs)
            grad_logits = (grad_capped * (1.0 - tanh_z * tanh_z)).astype(jnp.bfloat16)
            grad_logits = lax.optimization_barrier(grad_logits)
            part_dn = jnp.dot(grad_logits, table, preferred_element_type=jnp.float32)
            own_dn.append(lax.psum_scatter(part_dn, 'pp', scatter_dimension=0, tiled=True))
            table_part = lax.dot_general(grad_logits, block, (((0,), (0,)), ((), ())), preferred_element_type=jnp.float32)
            grad_table = table_part if grad_table is None else grad_table + table_part
            own_loss.append(lax.dynamic_slice_in_dim(tok_loss, rank * part, part, axis=0))
            loss_sum = loss_sum + jnp.sum(tok_loss)

        grad_rows, grad_gain = norm_vjp(jnp.concatenate(own_dn, axis=0))
        grad_gain = lax.psum(grad_gain, 'pp')
        loss = jnp.concatenate(own_loss).reshape(mb_dev, seq_len)
        mean_loss = jnp.reshape(loss_sum / total, (1,))
        return loss, grad_rows.astype(jnp.bfloat16).reshape(hidden.shape), mean_loss, grad_table, grad_gain

    token_spec = P(('dp', 'pp'))
    return jax.shard_map(local_fn, mesh=mesh,
                         in_specs=(token_spec, token_spec, P(), P('pp')),
                         out_specs=(token_spec, token_spec, P('dp'), token_spec, P('dp')),
                         check_vma=False)
```
